32 devices in a mesh: groups: 1, role: 2 (over core), dev: 16 (over z, y, x).
Axes of the slice: x: 2, y: 2, z: 4, core: 2. Of those that a mesh axis runs over, the one named last changes fastest.
Arguments:
- prompt_hidden: bfloat16 [4096, 4096], P(('groups', 'dev')), may hold values from -6 to 6
- norm_gain: float32 [4096], replicated, may hold values from 0.25 to 1.75
- kv_weight: bfloat16 [4096, 4, 2, 128], P(None, 'role'), may hold values from -0.09375 to 0.09375
- prompt_excess: int32 [4], P('groups'), may hold values from 1 to 1536, 2048 in all
- prompt_owner: int32 [4], P('groups'), may hold values from 0 to 15, as said below
- response_counts: int32 [4], P('groups'), may hold values from 1 to 5, as said below
- queries: bfloat16 [256, 16, 128], P(('groups', 'dev'), 'role'), may hold values from -256 to 256
- new_kv: bfloat16 [256, 4, 2, 128], P(('groups', 'dev'), 'role'), may hold values from -6 to 6
- response_cache: bfloat16 [256, 256, 4, 2, 128], P(('groups', 'dev'), None, 'role'), may hold values from -6 to 6
- positions: int32 [256], P(('groups', 'dev')), may hold values from 0 to 256
- out_weight: bfloat16 [16, 128, 4096], P('role', None, 'dev'), may hold values from -0.125 to 0.125
Outputs:
- attended: bfloat16 [256, 16, 128], P(('groups', 'dev'), 'role')
- block_out: bfloat16 [256, 4096], P(('groups', 'role'), 'dev')
The draws below stay inside these ranges and needn't reach their ends.
Inputs may be any that keep to these rules, and one draw needn't show every extreme that they name: `prompt_owner`: no device along dev owns more than two prompts, and some device owns exactly two. `response_counts`: some prompt has exactly 5 responses.
All inputs are finite; a program needn't handle non-finite values.
Results may differ from the reference program's by a relative error of at most 0.0065.
Values may be sent and summed in bfloat16 or wider, within the bound.
No kernel may reach another device: no remote copies, remote signals or barrier semaphores. Data moves between devices by JAX's collectives and lax.ppermute only.
A program may use at most 192 MiB of HBM per device.

```python
import math
import jax
import jax.numpy as jnp
import numpy as np
from jax import lax

D = 4096
HEAD = 128
KV_HEADS = 4
Q_HEADS = 16
RESP = 5
PROMPT_MIN = 512
SEQ_DEV = 16
CTX = 256
TOKENS = 4096
PROMPTS = 4
LONGEST = 2048
SEQS = 256
N_DEV = 16


def owners_counts(key):
    folded = jax.random.fold_in(key, 11)
    seat_key, order_key, count_key, place_key = jax.random.split(folded, 4)
    seating = jax.random.permutation(seat_key, 2 * N_DEV).astype(jnp.int32)
    partner = jnp.bitwise_xor(seating[0], 1)
    where_partner = jnp.argmax(seating == partner)
    seating = seating.at[where_partner].set(seating[1])
    seating = seating.at[1].set(partner)
    chosen = seating[:PROMPTS] // 2
    picked = chosen[2] if PROMPTS > 2 else chosen[0]
    last_device = N_DEV - 1
    chosen = jnp.where(chosen == picked, last_device, jnp.where(chosen == last_device, picked, chosen))
    shuffle = jax.random.permutation(order_key, PROMPTS)
    owners = chosen[shuffle].astype(jnp.int32)
    counts = jax.random.randint(count_key, (PROMPTS,), 1, RESP + 1)
    placed = jax.random.randint(place_key, (), 0, PROMPTS)
    counts = counts.at[placed].set(RESP)
    return (owners, counts.astype(jnp.int32))


def draw_prompt_owner(key, part):
    return owners_counts(key)[0]


def draw_response_counts(key, part):
    return owners_counts(key)[1]


def draw_queries(key, part):
    values = jax.random.normal(key, (SEQS, Q_HEADS, HEAD), jnp.float32)
    values = jnp.clip(values, -4.0, 4.0)
    return values.astype(jnp.bfloat16)


def with_ends(result, own_key, smallest, largest):
    dims = result.shape
    index_at = [jax.random.randint(jax.random.fold_in(own_key, axis), (), 0, dims[axis]) for axis in range(len(dims))]
    result = result.at[tuple(index_at)].set(smallest)
    longest = dims.index(max(dims))
    index_at[longest] = (index_at[longest] + 1) % dims[longest]
    return result.at[tuple(index_at)].set(largest)


def levels(own_key, dims, cuts, least, high):
    gain = 1.0
    for dim, shards_of in cuts:
        heights = jax.random.uniform(jax.random.fold_in(jax.random.fold_in(own_key, 6), dim), (shards_of,), jnp.float32, least / len(cuts), high / len(cuts))
        gain = gain * jnp.repeat(jnp.exp(heights), dims[dim] // shards_of).reshape((-1,) + (1,) * (len(dims) - 1 - dim))
    return gain


def length_profile(number_of, total, reach, slope):
    loads = [(1 << 20) // math.isqrt(rank ** slope) + 1 for rank in range(2, number_of + 1)]
    surplus, holding = total - reach - (number_of - 1), [1] * (number_of - 1)
    while surplus > 0:
        candidates = [i for i in range(number_of - 1) if holding[i] < reach]
        mass, budget = sum([loads[i] for i in candidates]), surplus
        for i in candidates:
            addition = min(reach - holding[i], max(1, budget * loads[i] // mass), surplus)
            holding[i] = holding[i] + addition
            surplus = surplus - addition
    return np.array([reach] + holding)


def ragged(key, number_of, total, reach, skew):
    if number_of == 2:
        one = jax.random.randint(key, (), max(1, total - reach), min(reach, total - 1) + 1)
        return jnp.stack([one, total - one])
    sizes = jnp.asarray(length_profile(number_of, total, reach, skew), jnp.int32)
    pairs = (number_of - 1) // 2
    source_of, sink = sizes[1:1 + 2 * pairs:2], sizes[2:2 + 2 * pairs:2]
    margin = jnp.minimum(source_of - 1, reach - sink)
    passed = jax.random.randint(jax.random.fold_in(key, 1), (pairs,), 0, 1 << 20) % (margin + 1)
    sizes = sizes.at[1:1 + 2 * pairs:2].set(source_of - passed).at[2:2 + 2 * pairs:2].set(sink + passed)
    return sizes[jax.random.permutation(jax.random.fold_in(key, 2), number_of)]


def normal_values(key, dims, spread, most, cuts=(), kind=jnp.bfloat16):
    gain = levels(key, dims, cuts, -0.22, 0.18) if cuts else 1.0
    values = jax.random.normal(key, dims, jnp.float32) * spread * gain
    return jnp.minimum(jnp.maximum(values, -most), most).astype(kind)


def setup_inputs(seed: int = 0, part: int = 0) -> dict:
    key_of = jax.random.split(jax.random.key(seed), 12)
    own_keys = jax.random.split(jax.random.fold_in(key_of[11], part), 12)
    return {
        "prompt_hidden": normal_values(own_keys[0], (TOKENS, D), 1.0, 6.0, ((0, 16),)),
        "norm_gain": jnp.clip(1.0 + 0.15 * jax.random.normal(key_of[1], (D,), jnp.float32), 0.25, 1.75),
        "kv_weight": normal_values(key_of[2], (D, KV_HEADS, 2, HEAD), D ** -0.5, 0.09375, ((1, 2),)),
        "prompt_excess": ragged(own_keys[3], PROMPTS, TOKENS - PROMPTS * PROMPT_MIN, LONGEST - PROMPT_MIN, 2).astype(jnp.int32),
        "prompt_owner": draw_prompt_owner(jax.random.fold_in(jax.random.fold_in(key_of[11], part), 71), part),
        "response_counts": draw_response_counts(jax.random.fold_in(jax.random.fold_in(key_of[11], part), 71), part),
        "queries": draw_queries(jax.random.fold_in(jax.random.fold_in(key_of[11], part), 71), part),
        "new_kv": normal_values(own_keys[7], (SEQS, KV_HEADS, 2, HEAD), 1.0, 6.0, ((0, 16), (1, 2))),
        "response_cache": normal_values(own_keys[8], (SEQS, CTX, KV_HEADS, 2, HEAD), 1.0, 6.0, ((0, 16), (2, 2))),
        "positions": with_ends(jax.random.randint(own_keys[9], (SEQS,), 0, CTX + 1), jax.random.fold_in(own_keys[9], 1), 0, CTX).astype(jnp.int32),
        "out_weight": normal_values(key_of[10], (Q_HEADS, HEAD, D), (Q_HEADS * HEAD) ** -0.5, 0.125, ((0, 2), (2, 16))),
    }


rope_base = 500000.0

def rotate(vectors, offsets):
    half = vectors.shape[-1] // 2
    freq = rope_base ** (-jnp.arange(half, dtype=jnp.float32) * 2.0 / vectors.shape[-1])
    angles = offsets.astype(jnp.float32)[:, None] * freq[None, :]
    cosine = jnp.cos(angles)[:, None, :]
    sine = jnp.sin(angles)[:, None, :]
    first = vectors[..., :half]
    second = vectors[..., half:]
    return jnp.concatenate([first * cosine - second * sine, second * cosine + first * sine], axis=-1)

def prompt_layout(prompt_excess, token_index):
    lengths = PROMPT_MIN + prompt_excess
    ends = jnp.cumsum(lengths).astype(jnp.int32)
    starts = (ends - lengths).astype(jnp.int32)
    prompt_id = lax.optimization_barrier(jnp.sum((token_index[:, None] >= ends[None, :]).astype(jnp.int32), axis=1))
    member = prompt_id[:, None] == jnp.arange(lengths.shape[0], dtype=jnp.int32)[None, :]
    offsets = token_index - lax.optimization_barrier(jnp.sum(jnp.where(member, starts[None, :], 0), axis=1))
    return (member, offsets, starts, lengths)

def slot_prompts(owner, counts, slot_device, slot_index):
    order = jnp.arange(owner.shape[0], dtype=jnp.int32)
    earlier = (owner[:, None] == owner[None, :]) & (order[None, :] < order[:, None])
    first = lax.optimization_barrier(jnp.sum(jnp.where(earlier, counts[None, :], 0), axis=1))
    match = (owner[None, :] == slot_device[:, None]) & (first[None, :] <= slot_index[:, None]) & (slot_index[:, None] < first[None, :] + counts[None, :])
    present = jnp.any(match, axis=1)
    chosen = lax.optimization_barrier(jnp.sum(jnp.where(match, order[None, :], 0), axis=1)).astype(jnp.int32)
    return (chosen, present)

def reference(prompt_hidden, norm_gain, kv_weight, prompt_excess, prompt_owner, response_counts, queries, new_kv, response_cache, positions, out_weight):
    token_index = jnp.arange(TOKENS, dtype=jnp.int32)
    member, offsets, starts, lengths = prompt_layout(prompt_excess, token_index)
    hidden = prompt_hidden.astype(jnp.float32)
    normed = (hidden * lax.rsqrt(lax.optimization_barrier(jnp.mean(hidden * hidden, axis=-1, keepdims=True)) + 1e-05) * norm_gain).astype(jnp.bfloat16)
    projected = jnp.dot(normed, kv_weight.reshape(D, KV_HEADS * 2 * HEAD), preferred_element_type=jnp.float32)
    projected = projected.reshape(TOKENS, KV_HEADS, 2, HEAD)
    prompt_keys = rotate(projected[:, :, 0], offsets).astype(jnp.bfloat16)
    prompt_values = projected[:, :, 1].astype(jnp.bfloat16)
    slot_all = jnp.arange(SEQS, dtype=jnp.int32)
    chosen, present = slot_prompts(prompt_owner, response_counts, slot_all // SEQ_DEV, slot_all % SEQ_DEV)
    group = Q_HEADS // KV_HEADS

    def one_slot(inputs):
        query, fresh, cache, position, pick, live = inputs
        begin = jnp.minimum(starts[pick], TOKENS - LONGEST).astype(jnp.int32)
        window_keys = lax.dynamic_slice_in_dim(prompt_keys, begin, LONGEST, 0)
        window_values = lax.dynamic_slice_in_dim(prompt_values, begin, LONGEST, 0)
        token_ids = begin + jnp.arange(LONGEST, dtype=jnp.int32)
        prompt_valid = live & (token_ids >= starts[pick]) & (token_ids < starts[pick] + lengths[pick])
        cache_valid = jnp.arange(CTX, dtype=jnp.int32) < position
        all_keys = jnp.concatenate([window_keys, cache[:, :, 0], fresh[None, :, 0]], axis=0)
        all_values = jnp.concatenate([window_values, cache[:, :, 1], fresh[None, :, 1]], axis=0)
        valid = jnp.concatenate([prompt_valid, cache_valid, jnp.ones((1,), dtype=bool)], axis=0)
        grouped = query.astype(jnp.float32).reshape(KV_HEADS, group, HEAD)
        scores = jnp.einsum('ngd,lnd->ngl', grouped, all_keys.astype(jnp.float32)) * HEAD ** (-0.5)
        scores = jnp.where(valid[None, None, :], scores, -1e+30)
        peak = lax.optimization_barrier(jnp.max(scores, axis=-1, keepdims=True))
        weights = jnp.where(valid[None, None, :], jnp.exp(scores - peak), 0.0)
        total = lax.optimization_barrier(jnp.sum(weights, axis=-1))
        rounded = lax.optimization_barrier(weights.astype(jnp.bfloat16)).astype(jnp.float32)
        mixed = jnp.einsum('ngl,lnd->ngd', rounded, all_values.astype(jnp.float32))
        return (mixed / total[..., None]).reshape(Q_HEADS, HEAD).astype(jnp.bfloat16)
    attended = lax.map(one_slot, (queries, new_kv, response_cache, positions, chosen, present))
    block_out = jnp.dot(attended.reshape(SEQS, Q_HEADS * HEAD), out_weight.reshape(Q_HEADS * HEAD, D), preferred_element_type=jnp.float32).astype(jnp.bfloat16)
    return (attended, block_out)
```

```python
import functools

import jax
import jax.numpy as jnp
import numpy as np
from jax import lax
from jax.experimental import pallas as pl
from jax.experimental.pallas import tpu as pltpu
from jax.sharding import PartitionSpec as P

RESP = 5
PROMPT_MIN = 512
ROPE_BASE = 500000.0
EPS = 1e-05
LOW = -1e30
LANES = 128

SMEM = pl.BlockSpec(memory_space=pltpu.SMEM)
VMEM = pl.BlockSpec(memory_space=pltpu.VMEM)
ANY = pl.BlockSpec(memory_space=pl.ANY)
NT = (((1,), (1,)), ((), ()))
NN = (((1,), (0,)), ((), ()))


def cost(flops, bytes_accessed):
    return pl.CostEstimate(flops=flops, bytes_accessed=bytes_accessed, transcendentals=0)


def params(mib=48):
    return pltpu.CompilerParams(vmem_limit_bytes=mib << 20)


def phases(n):
    found, stride = [], 1
    while n > 1:
        radix = 4 if n % 4 == 0 else 2
        assert n % radix == 0
        found.append((stride, radix))
        stride, n = stride * radix, n // radix
    return found


def exchange(x, phase):
    stride, radix = phase
    n = lax.axis_size("dev")
    return [
        lax.ppermute(x, "dev", [(i, i ^ (k * stride)) for i in range(n)]) for k in range(1, radix)
    ]


def dot(a, b, dims):
    return lax.dot_general(a, b, dims, preferred_element_type=jnp.float32)


def first_slot(owner, counts, p):
    total = jnp.int32(0)
    for q in range(p):
        total = total + jnp.where(owner[q] == owner[p], counts[q], 0)
    return total


def digit(index, phase):
    stride, radix = phase
    return lax.rem(lax.div(index, stride), radix)


def cache_kernel(per, pos_ref, q_ref, new_ref, cache_ref, out_ref, o_ref, lse_ref, att):
    slots, heads, size = q_ref.shape
    ways = new_ref.shape[1]
    group = heads // (ways // 2)
    rows = cache_ref.shape[1]
    scale = size ** (-0.5)
    step = pl.program_id(0)
    head = lax.broadcasted_iota(jnp.int32, (heads, 1), 0) // group
    column = lax.broadcasted_iota(jnp.int32, (heads, rows), 1)
    mine = (column % ways) == 2 * head
    for i in range(per):
        s = step * per + i
        q = q_ref[s]
        scores = dot(q, cache_ref[i], NT) * scale
        valid = mine & (column < pos_ref[s] * ways)
        scores = jnp.where(valid, scores, LOW)
        fresh = new_ref[s].astype(jnp.float32)
        key = jnp.zeros((heads, size), jnp.float32)
        value = jnp.zeros((heads, size), jnp.float32)
        for n in range(ways // 2):
            key = jnp.where(head == n, fresh[2 * n : 2 * n + 1, :], key)
            value = jnp.where(head == n, fresh[2 * n + 1 : 2 * n + 2, :], value)
        own = jnp.sum(q.astype(jnp.float32) * key, axis=1, keepdims=True) * scale
        peak = jnp.maximum(jnp.max(scores, axis=1, keepdims=True), own)
        weights = jnp.where(valid, jnp.exp(scores - peak), 0.0)
        alone = jnp.exp(own - peak)
        total = jnp.sum(weights, axis=1, keepdims=True) + alone
        moved = pltpu.roll(weights, 1, axis=1).astype(jnp.bfloat16)
        mixed = dot(moved, cache_ref[i], NN)
        mixed = mixed + alone.astype(jnp.bfloat16).astype(jnp.float32) * value
        mixed = mixed / total
        o_ref[s] = mixed
        lse_ref[s] = jnp.broadcast_to(peak + jnp.log(total), (heads, size))
        att[pl.ds(s, heads, stride=slots), :] = mixed

    @pl.when(step == pl.num_programs(0) - 1)
    def _():
        out_ref[...] = att[...].astype(out_ref.dtype)


def cache_attention(positions, queries, new_kv, response_cache):
    slots, heads, size = queries.shape
    ctx, kv = response_cache.shape[1], response_cache.shape[2]
    rows = ctx * kv * 2
    per = 2
    whole = lambda *shape: pl.BlockSpec(shape, lambda i: (0,) * len(shape))
    f32 = jnp.float32
    return pl.pallas_call(
        functools.partial(cache_kernel, per),
        grid=(slots // per,),
        in_specs=[
            SMEM,
            whole(slots, heads, size),
            whole(slots, kv * 2, size),
            pl.BlockSpec((per, rows, size), lambda i: (i, 0, 0)),
        ],
        out_specs=[
            whole(slots * heads, size),
            whole(slots, heads, size),
            whole(slots, heads, size),
        ],
        out_shape=[
            jax.ShapeDtypeStruct((slots * heads, size), jnp.bfloat16),
            jax.ShapeDtypeStruct((slots, heads, size), f32),
            jax.ShapeDtypeStruct((slots, heads, size), f32),
        ],
        scratch_shapes=[pltpu.VMEM((slots * heads, size), f32)],
        compiler_params=params(),
        cost_estimate=cost(10_000_000_000, slots * rows * size * 2),
        name="cache_attention",
    )(
        positions,
        queries,
        new_kv.reshape(slots, kv * 2, size),
        response_cache.reshape(slots, rows, size),
    )


def project_kernel(
    chunks, excess, hid_hbm, gain_ref, freq_ref, w_hbm, k_ref, v_ref, hid, w, wide, acc, hsem, wsem
):
    rows, width = hid.shape
    size = w.shape[1]
    ways = w.shape[0] // width
    depth = width // chunks
    load = pltpu.make_async_copy(hid_hbm, hid, hsem)
    load.start()
    loads = []
    for c in range(chunks):
        part = pl.ds(c * depth * ways, depth * ways)
        loads.append(pltpu.make_async_copy(w_hbm.at[part, :], w.at[part, :], wsem.at[c]))
        loads[-1].start()
    token = lax.axis_index("dev") * rows + lax.broadcasted_iota(jnp.int32, (rows, size), 0)
    offset, start = token, jnp.int32(0)
    for p in range(excess.shape[0]):
        offset = jnp.where(token >= start, token - start, offset)
        start = start + PROMPT_MIN + excess[p]
    angle = offset.astype(jnp.float32) * freq_ref[...]
    lane = lax.broadcasted_iota(jnp.int32, (rows, size), 1)
    cosine = jnp.cos(angle)
    sine = jnp.where(lane < size // 2, -1.0, 1.0) * jnp.sin(angle)
    load.wait()
    total = jnp.zeros((rows, 1), jnp.float32)
    for c in range(chunks):
        x = hid[:, c * depth : (c + 1) * depth].astype(jnp.float32)
        total = total + jnp.sum(x * x, axis=1, keepdims=True)
    inverse = lax.rsqrt(total / width + EPS)
    for c in range(chunks):
        at = slice(c * depth, (c + 1) * depth)
        x = hid[:, at].astype(jnp.float32) * inverse * gain_ref[:, at]
        x = x.astype(jnp.bfloat16)
        loads[c].wait()
        buffer = wide.at[c % 2]
        buffer[...] = w[c * depth * ways : (c + 1) * depth * ways, :].astype(jnp.float32)
        parts = [
            buffer[pl.ds(j, depth, stride=ways), :].astype(jnp.bfloat16) for j in range(ways)
        ]
        term = dot(x, jnp.concatenate(parts, axis=1), NN)
        if c == 0:
            acc[...] = term
        else:
            acc[...] += term
    for n in range(ways // 2):
        key = acc[:, 2 * n * size : (2 * n + 1) * size]
        turned = key * cosine + pltpu.roll(key, size // 2, axis=1) * sine
        k_ref[n] = turned.astype(k_ref.dtype)
        v_ref[n] = acc[:, (2 * n + 1) * size : (2 * n + 2) * size].astype(v_ref.dtype)


def project(prompt_hidden, norm_gain, kv_weight, prompt_excess):
    rows, width = prompt_hidden.shape
    kv, size = kv_weight.shape[1], kv_weight.shape[3]
    ways = kv * 2
    chunks = 8
    depth = width // chunks
    half = np.arange(size // 2, dtype=np.float64)
    freq = ROPE_BASE ** (-2.0 * half / size)
    freq = jnp.asarray(np.concatenate([freq, freq])[None, :], jnp.float32)
    f32, bf16 = jnp.float32, jnp.bfloat16
    return pl.pallas_call(
        functools.partial(project_kernel, chunks),
        in_specs=[SMEM, ANY, VMEM, VMEM, ANY],
        out_specs=[VMEM, VMEM],
        out_shape=[jax.ShapeDtypeStruct((kv, rows, size), bf16)] * 2,
        scratch_shapes=[
            pltpu.VMEM((rows, width), bf16),
            pltpu.VMEM((width * ways, size), bf16),
            pltpu.VMEM((2, depth * ways, size), f32),
            pltpu.VMEM((rows, ways * size), f32),
            pltpu.SemaphoreType.DMA,
            pltpu.SemaphoreType.DMA((chunks,)),
        ],
        compiler_params=params(),
        cost_estimate=cost(10_000_000_000, width * (rows + ways * size) * 2),
        name="project",
    )(
        prompt_excess,
        prompt_hidden,
        norm_gain[None, :],
        freq,
        kv_weight.reshape(width * ways, size),
    )


def pick_tile(refs, owner, phase, index):
    own = digit(lax.axis_index("dev"), phase)
    tile = refs[0][index]
    for k in range(1, len(refs)):
        tile = jnp.where(digit(owner, phase) == jnp.bitwise_xor(own, k), refs[k][index], tile)
    return tile


def slot_of(owner, counts, p, r, slots):
    return jnp.minimum(first_slot(owner, counts, p) + r, slots - 1)


def table_kernel(phase, raw, carried, owner, counts, *refs):
    radix = phase[1]
    sources, out = refs[:radix], refs[-1]
    entries = owner.shape[0] * RESP
    slots = sources[0].shape[0]
    for p in range(owner.shape[0]):
        for r in range(RESP):
            index = slot_of(owner, counts, p, r, slots) if raw else p * RESP + r
            out[p * RESP + r] = pick_tile(sources, owner[p], phase, index)
    at = entries
    if raw:
        local = refs[radix]
        out[at : at + local.shape[0]] = local[...]
    else:
        for source in sources:
            out[at : at + carried] = source[entries : entries + carried]
            at += carried


def make_table(phase, raw, carried, owner, counts, sources, local):
    heads, size = sources[0].shape[1:]
    entries = owner.shape[0] * RESP
    extra = local.shape[0] if raw else carried * len(sources)
    args = list(sources) + ([local] if raw else [])
    return pl.pallas_call(
        functools.partial(table_kernel, phase, raw, carried),
        in_specs=[SMEM, SMEM] + [VMEM] * len(args),
        out_specs=VMEM,
        out_shape=jax.ShapeDtypeStruct((entries + extra, heads, size), sources[0].dtype),
        compiler_params=params(),
        cost_estimate=cost(100_000_000, 200_000),
        name="make_table",
    )(owner, counts, *args)


def stat_rows(rows):
    return 16 * pl.cdiv(3 * pl.cdiv(rows, LANES), 16)


def put_state(out, mixed, lse, rows):
    out[:rows, :] = mixed.astype(out.dtype)
    count = pl.cdiv(rows, LANES)
    line = lax.broadcasted_iota(jnp.int32, (LANES, LANES), 0)
    lane = lax.broadcasted_iota(jnp.int32, (LANES, LANES), 1)
    place = lax.broadcasted_iota(jnp.int32, (stat_rows(rows), LANES), 0)
    stats = jnp.zeros((stat_rows(rows), LANES), jnp.float32)
    for b in range(count):
        size = min(LANES, rows - b * LANES)
        eye = line[:size] == lane[:size]
        rest = jnp.sum(
            jnp.where(eye, lse[b * LANES : b * LANES + size, :], 0.0), axis=0, keepdims=True
        )
        for k in range(3):
            term = rest.astype(jnp.bfloat16).astype(jnp.float32)
            stats = jnp.where(place == 3 * b + k, term, stats)
            rest = rest - term
    out[rows : rows + stat_rows(rows), :] = stats.astype(out.dtype)


def get_lse(message, rows):
    stats = message[rows : rows + stat_rows(rows), :].astype(jnp.float32)
    line = lax.broadcasted_iota(jnp.int32, (LANES, LANES), 0)
    lane = lax.broadcasted_iota(jnp.int32, (LANES, LANES), 1)
    blocks = []
    for b in range(pl.cdiv(rows, LANES)):
        size = min(LANES, rows - b * LANES)
        row = (stats[3 * b : 3 * b + 1] + stats[3 * b + 1 : 3 * b + 2]) + stats[3 * b + 2 : 3 * b + 3]
        eye = line[:size] == lane[:size]
        blocks.append(jnp.sum(jnp.where(eye, row, 0.0), axis=1, keepdims=True))
    return jnp.concatenate(blocks, axis=0) if len(blocks) > 1 else blocks[0]


def merge(messages, rows):
    lses = [get_lse(m, rows) for m in messages]
    peak = functools.reduce(jnp.maximum, lses)
    total = jnp.zeros_like(peak)
    mixed = None
    for m, lse in zip(messages, lses):
        weight = jnp.exp(lse - peak)
        total = total + weight
        term = m[:rows, :].astype(jnp.float32) * weight
        mixed = term if mixed is None else mixed + term
    return mixed / total, peak + jnp.log(total)


def prompt_kernel(
    phase, raw, carried, excess, owner, counts, k_ref, v_ref, o_ref, lse_ref, *refs
):
    radix = phase[1]
    sources, out, table, mine_o, mine_lse = refs[:radix], refs[-4], refs[-3], refs[-2], refs[-1]
    kv, tokens, size = k_ref.shape
    slots, heads, _ = o_ref.shape
    group = heads // kv
    prompts = owner.shape[0]
    rows = prompts * RESP * heads
    me = lax.axis_index("dev")
    for p in range(prompts):
        here = owner[p] == me
        for r in range(RESP):
            t = p * RESP + r
            slot = slot_of(owner, counts, p, r, slots)
            tile = pick_tile(sources, owner[p], phase, slot if raw else t)
            table[t * heads : (t + 1) * heads, :] = tile.astype(jnp.float32)
            mine_o[t * heads : (t + 1) * heads, :] = o_ref[slot]
            mine_lse[t * heads : (t + 1) * heads, :] = jnp.where(here, lse_ref[slot], LOW)
    queries = table[...].astype(jnp.bfloat16)
    head = (lax.broadcasted_iota(jnp.int32, (rows, 1), 0) % heads) // group
    scores = dot(queries, k_ref[0], NT)
    for n in range(1, kv):
        scores = jnp.where(head == n, dot(queries, k_ref[n], NT), scores)
    token = me * tokens + lax.broadcasted_iota(jnp.int32, (1, tokens), 1)
    start = jnp.int32(0)
    valid = []
    for p in range(prompts):
        end = start + PROMPT_MIN + excess[p]
        inside = ((token >= start) & (token < end)).astype(jnp.float32)
        valid.append(jnp.broadcast_to(inside, (RESP * heads, tokens)))
        start = end
    valid = jnp.concatenate(valid, axis=0) > 0.5
    scores = jnp.where(valid, scores * size ** (-0.5), LOW)
    peak = jnp.max(scores, axis=1, keepdims=True)
    weights = jnp.where(valid, jnp.exp(scores - peak), 0.0)
    total = jnp.sum(weights, axis=1, keepdims=True)
    weights = weights.astype(jnp.bfloat16)
    mixed = dot(weights, v_ref[0], NN)
    for n in range(1, kv):
        mixed = jnp.where(head == n, dot(weights, v_ref[n], NN), mixed)
    other = mine_lse[...]
    top = jnp.maximum(other, peak)
    left = jnp.exp(peak - top)
    right = jnp.exp(other - top)
    total = total * left + right
    mixed = (mixed * left + mine_o[...] * right) / total
    put_state(out, mixed, top + jnp.log(total), rows)
    at = rows + stat_rows(rows)
    entries = prompts * RESP
    for source in sources:
        block = source[entries : entries + carried] if not raw else source[...]
        out[at : at + carried * heads, :] = block.reshape(carried * heads, size)
        at += carried * heads


def prompt_attention(phase, carried, excess, owner, counts, keys, values, o, lse, sources):
    heads, size = o.shape[1:]
    rows = owner.shape[0] * RESP * heads
    total = rows + stat_rows(rows) + carried * heads * len(sources)
    f32 = jnp.float32
    return pl.pallas_call(
        functools.partial(prompt_kernel, phase, False, carried),
        in_specs=[SMEM] * 3 + [VMEM] * (4 + len(sources)),
        out_specs=VMEM,
        out_shape=jax.ShapeDtypeStruct((total, size), jnp.bfloat16),
        scratch_shapes=[pltpu.VMEM((rows, size), f32)] * 3,
        compiler_params=params(),
        cost_estimate=cost(2_000_000_000, 500_000),
        name="prompt_attention",
    )(excess, owner, counts, keys, values, o, lse, *sources)


def merge_kernel(rows, *refs):
    mixed, lse = merge(refs[:-1], rows)
    put_state(refs[-1], mixed, jnp.broadcast_to(lse, mixed.shape), rows)


def merge_states(rows, messages):
    size = messages[0].shape[1]
    return pl.pallas_call(
        functools.partial(merge_kernel, rows),
        in_specs=[VMEM] * len(messages),
        out_specs=VMEM,
        out_shape=jax.ShapeDtypeStruct((rows + stat_rows(rows), size), jnp.bfloat16),
        compiler_params=params(),
        cost_estimate=cost(1_000_000_000, 500_000),
        name="merge_states",
    )(*messages)


def base_kernel(offsets, skip, slots, w_ref, *refs):
    sources, keep, give, lhs = refs[:-3], refs[-3], refs[-2], refs[-1]
    heads, size, _ = w_ref.shape
    me = lax.axis_index("dev")
    block = slots * heads
    per = len(offsets) // len(sources)
    for i, offset in enumerate(offsets):
        at = pl.multiple_of(jnp.bitwise_xor(me, offset) * slots, slots)
        begin = skip + (i % per) * block
        for h in range(heads):
            lhs[pl.ds(at, slots), h * size : (h + 1) * size] = sources[i // per][
                begin + h * slots : begin + (h + 1) * slots, :
            ]
    half = keep.shape[0]
    role = lax.axis_index("role")
    weight = w_ref[...].reshape(heads * size, w_ref.shape[2])
    keep[...] = dot(lhs[pl.ds(pl.multiple_of(role * half, half), half), :], weight, NN)
    give[...] = dot(lhs[pl.ds(pl.multiple_of((1 - role) * half, half), half), :], weight, NN)


def base_product(offsets, skip, slots, weight, sources):
    heads, size, columns = weight.shape
    total = len(offsets) * slots
    half = jax.ShapeDtypeStruct((total // 2, columns), jnp.float32)
    return pl.pallas_call(
        functools.partial(base_kernel, offsets, skip, slots),
        in_specs=[VMEM] * (1 + len(sources)),
        out_specs=[VMEM, VMEM],
        out_shape=[half, half],
        scratch_shapes=[pltpu.VMEM((total, heads * size), jnp.bfloat16)],
        compiler_params=params(),
        cost_estimate=cost(2_000_000_000, 1_000_000),
        name="base_product",
    )(weight, *sources)


def answer_kernel(rows, owner, counts, w_ref, o_ref, *refs):
    messages, att_ref, part, joined = refs[:-3], refs[-3], refs[-2], refs[-1]
    heads, size, columns = w_ref.shape
    slots = o_ref.shape[0]
    entries = rows // heads
    mixed, _ = merge(messages, rows)
    joined[...] = mixed
    att_ref[...] = o_ref[...].astype(att_ref.dtype)
    me = lax.axis_index("dev")
    for p in range(owner.shape[0]):
        for r in range(RESP):
            t = p * RESP + r

            @pl.when((owner[p] == me) & (r < counts[p]))
            def _():
                tile = joined[t * heads : (t + 1) * heads, :]
                att_ref[slot_of(owner, counts, p, r, slots)] = tile.astype(att_ref.dtype)

    total = None
    for h in range(heads):
        lhs = joined[pl.ds(h, entries, stride=heads), :].astype(jnp.bfloat16)
        term = dot(lhs, w_ref[h], NN)
        total = term if total is None else total + term
    part[:entries, :] = total


def answer_product(rows, owner, counts, weight, o, messages):
    heads, size, columns = weight.shape
    entries = rows // heads
    return pl.pallas_call(
        functools.partial(answer_kernel, rows),
        in_specs=[SMEM, SMEM] + [VMEM] * (2 + len(messages)),
        out_specs=[VMEM, VMEM],
        out_shape=[
            jax.ShapeDtypeStruct(o.shape, jnp.bfloat16),
            jax.ShapeDtypeStruct((8 * pl.cdiv(entries, 8), columns), jnp.float32),
        ],
        scratch_shapes=[pltpu.VMEM((rows, size), jnp.float32)],
        compiler_params=params(),
        cost_estimate=cost(1_000_000_000, 1_000_000),
        name="answer_product",
    )(owner, counts, weight, o, *messages)


def finish_kernel(slots, owner, counts, keep, taken, part, part_taken, out, wide):
    half = keep.shape[0]
    begin = lax.axis_index("role") * half
    wide[...] = keep[...] + taken[...]
    for p in range(owner.shape[0]):
        for r in range(RESP):
            t = p * RESP + r
            row = owner[p] * slots + slot_of(owner, counts, p, r, slots) - begin

            @pl.when((r < counts[p]) & (row >= 0) & (row < half))
            def _():
                wide[pl.ds(row, 1), :] = part[t : t + 1, :] + part_taken[t : t + 1, :]

    out[...] = wide[...].astype(out.dtype)


def finish(slots, owner, counts, keep, taken, part, part_taken):
    return pl.pallas_call(
        functools.partial(finish_kernel, slots),
        in_specs=[SMEM, SMEM] + [VMEM] * 4,
        out_specs=VMEM,
        out_shape=jax.ShapeDtypeStruct(keep.shape, jnp.bfloat16),
        scratch_shapes=[pltpu.VMEM(keep.shape, jnp.float32)],
        compiler_params=params(),
        name="finish",
    )(owner, counts, keep, taken, part, part_taken)


def swap_role(x):
    return lax.ppermute(x, "role", [(0, 1), (1, 0)])


def on_device(
    prompt_hidden,
    norm_gain,
    kv_weight,
    excess,
    owner,
    counts,
    queries,
    new_kv,
    response_cache,
    positions,
    out_weight,
):
    slots, heads, size = queries.shape
    steps = phases(lax.axis_size("dev"))
    rows = owner.shape[0] * RESP * heads
    received = [queries] + exchange(queries, steps[0])
    local, o, lse = cache_attention(positions, queries, new_kv, response_cache)
    local = local.reshape(slots, heads, size)
    offsets = [0]
    carried = slots
    raw = True
    for before, phase in zip(steps[:-1], steps[1:]):
        message = make_table(before, raw, carried, owner, counts, received, local)
        received = [message] + exchange(message, phase)
        carried = carried if raw else carried * before[1]
        offsets = [k * phase[0] ^ a for k in range(phase[1]) for a in offsets]
        raw = False
    keys, values = project(prompt_hidden, norm_gain, kv_weight, excess)
    message = prompt_attention(
        steps[-1], carried, excess, owner, counts, keys, values, o, lse, received
    )
    received = [message] + exchange(message, steps[0])
    offsets = [k * steps[0][0] ^ a for k in range(steps[0][1]) for a in offsets]
    blocks = received
    for phase in steps[1:]:
        message = merge_states(rows, received)
        received = [message] + exchange(message, phase)
    keep, give = base_product(offsets, rows + stat_rows(rows), slots, out_weight, blocks)
    taken = swap_role(give)
    attended, part = answer_product(rows, owner, counts, out_weight, o, received)
    block_out = finish(slots, owner, counts, keep, taken, part, swap_role(part))
    return (attended, block_out)


def solution(mesh):
    return jax.shard_map(
        on_device,
        mesh=mesh,
        in_specs=(
            P(("groups", "dev"), None),
            P(),
            P(None, "role", None, None),
            P("groups"),
            P("groups"),
            P("groups"),
            P(("groups", "dev"), "role", None),
            P(("groups", "dev"), "role", None, None),
            P(("groups", "dev"), None, "role", None, None),
            P(("groups", "dev")),
            P("role", None, "dev"),
        ),
        out_specs=(P(("groups", "dev"), "role", None), P(("groups", "role"), "dev")),
        check_vma=False,
    )
```

```python
import functools

import jax
import jax.numpy as jnp
import numpy as np
from jax import lax
from jax.experimental import pallas as pl
from jax.experimental.pallas import tpu as pltpu
from jax.sharding import PartitionSpec as P

RESP = 5
PROMPT_MIN = 512
ROPE_BASE = 500000.0
EPS = 1e-05
LOW = -1e30
LANES = 128
CACHE_MIB = 24
CACHE_BLOCKS = 4

SMEM = pl.BlockSpec(memory_space=pltpu.SMEM)
VMEM = pl.BlockSpec(memory_space=pltpu.VMEM)
HBM = pl.BlockSpec(memory_space=pltpu.HBM)
NT = (((1,), (1,)), ((), ()))
NN = (((1,), (0,)), ((), ()))


def cost(flops, bytes_accessed):
    return pl.CostEstimate(flops=flops, bytes_accessed=bytes_accessed, transcendentals=0)


def params(mib=24):
    return pltpu.CompilerParams(vmem_limit_bytes=mib << 20)


def in_hbm(x):
    return pltpu.with_memory_space_constraint(x, pltpu.HBM)


def phases(n):
    found, stride = [], 1
    while n > 1:
        radix = 4 if n % 4 == 0 else 2
        assert n % radix == 0
        found.append((stride, radix))
        stride, n = stride * radix, n // radix
    return found


def exchange(x, phase):
    stride, radix = phase
    n = lax.axis_size("dev")
    return [
        lax.ppermute(x, "dev", [(i, i ^ (k * stride)) for i in range(n)]) for k in range(1, radix)
    ]


def dot(a, b, dims):
    return lax.dot_general(a, b, dims, preferred_element_type=jnp.float32)


def first_slot(owner, counts, p):
    total = jnp.int32(0)
    for q in range(p):
        total = total + jnp.where(owner[q] == owner[p], counts[q], 0)
    return total


def digit(index, phase):
    stride, radix = phase
    return lax.rem(lax.div(index, stride), radix)


def cache_kernel(
    pos_hbm, q_hbm, new_hbm, cache_hbm, hid_hbm, out_ref, o_ref, lse_ref, hid,
    att, table, key, value, pos, qs, fresh, cache, small, sems,
):
    slots, heads, size = qs.shape
    ways = fresh.shape[1]
    group = heads // (ways // 2)
    rows = cache.shape[1]
    scale = size ** (-0.5)
    blocks = sems.shape[0]
    block = slots // blocks
    first = [
        pltpu.make_async_copy(pos_hbm, pos, small.at[0]),
        pltpu.make_async_copy(q_hbm, qs, small.at[1]),
        pltpu.make_async_copy(new_hbm, fresh, small.at[2]),
    ]
    for load in first:
        load.start()
    loads = []
    for i in range(blocks):
        part = pl.ds(i * block, block)
        loads.append(pltpu.make_async_copy(cache_hbm.at[part], cache.at[part], sems.at[i]))
        loads[-1].start()
    extra = pltpu.make_async_copy(hid_hbm, hid, small.at[3])
    extra.start()
    for load in first:
        load.wait()
    head = lax.broadcasted_iota(jnp.int32, (heads, 1), 0) // group
    for s in range(slots):
        new = fresh[s].astype(jnp.float32)
        k = jnp.zeros((heads, size), jnp.float32)
        v = jnp.zeros((heads, size), jnp.float32)
        for n in range(ways // 2):
            k = jnp.where(head == n, new[2 * n : 2 * n + 1, :], k)
            v = jnp.where(head == n, new[2 * n + 1 : 2 * n + 2, :], v)
        key[s * heads : (s + 1) * heads, :] = qs[s].astype(jnp.float32) * k
        value[s * heads : (s + 1) * heads, :] = v
    line = lax.broadcasted_iota(jnp.int32, (block * heads, 1), 0)
    column = lax.broadcasted_iota(jnp.int32, (block * heads, rows), 1)
    mine = jnp.where((column % ways) == 2 * ((line % heads) // group), column, rows * ways)

    def score(i):
        for s in range(i * block, (i + 1) * block):
            table[s * heads : (s + 1) * heads, :] = dot(qs[s], cache[s], NT)

    def weigh(i):
        at = slice(i * block * heads, (i + 1) * block * heads)
        limit = jnp.zeros((block * heads, 1), jnp.int32)
        for j in range(block):
            limit = jnp.where(line // heads == j, pos[i * block + j] * ways, limit)
        valid = mine < limit
        scores = jnp.where(valid, table[at, :] * scale, LOW)
        own = jnp.sum(key[at, :], axis=1, keepdims=True) * scale
        peak = jnp.maximum(jnp.max(scores, axis=1, keepdims=True), own)
        weights = jnp.where(valid, jnp.exp(scores - peak), 0.0)
        alone = jnp.exp(own - peak)
        total = jnp.sum(weights, axis=1, keepdims=True) + alone
        table[at, :] = pltpu.roll(weights, 1, axis=1)
        return peak + jnp.log(total), alone.astype(jnp.bfloat16).astype(jnp.float32), total

    def mix(i, stats):
        for j in range(block):
            s = i * block + j
            at = slice(s * heads, (s + 1) * heads)
            mixed = dot(table[at, :].astype(jnp.bfloat16), cache[s], NN)
            lse, alone, total = (x[j * heads : (j + 1) * heads] for x in stats)
            mixed = (mixed + alone * value[at, :]) / total
            o_ref[s] = mixed
            lse_ref[s] = jnp.broadcast_to(lse, (heads, size))
            att[pl.ds(s, heads, stride=slots), :] = mixed

    stats = {}
    for i in range(blocks + 2):
        if i < blocks:
            loads[i].wait()
            score(i)
        if 0 <= i - 1 < blocks:
            stats[i - 1] = weigh(i - 1)
        if 0 <= i - 2:
            mix(i - 2, stats[i - 2])
    out_ref[...] = att[...].astype(out_ref.dtype)
    extra.wait()


def cache_attention(positions, queries, new_kv, response_cache, prompt_hidden):
    slots, heads, size = queries.shape
    ctx, kv = response_cache.shape[1], response_cache.shape[2]
    rows = ctx * kv * 2
    blocks = CACHE_BLOCKS if slots % CACHE_BLOCKS == 0 else 1
    f32, bf16 = jnp.float32, jnp.bfloat16
    return pl.pallas_call(
        cache_kernel,
        in_specs=[HBM] * 5,
        out_specs=[VMEM] * 4,
        out_shape=[
            jax.ShapeDtypeStruct((slots * heads, size), bf16),
            jax.ShapeDtypeStruct((slots, heads, size), f32),
            jax.ShapeDtypeStruct((slots, heads, size), f32),
            jax.ShapeDtypeStruct(prompt_hidden.shape, bf16),
        ],
        scratch_shapes=[
            pltpu.VMEM((slots * heads, size), f32),
            pltpu.VMEM((slots * heads, rows), f32),
            pltpu.VMEM((slots * heads, size), f32),
            pltpu.VMEM((slots * heads, size), f32),
            pltpu.SMEM((slots,), jnp.int32),
            pltpu.VMEM((slots, heads, size), bf16),
            pltpu.VMEM((slots, kv * 2, size), bf16),
            pltpu.VMEM((slots, rows, size), bf16),
            pltpu.SemaphoreType.DMA((4,)),
            pltpu.SemaphoreType.DMA((blocks,)),
        ],
        compiler_params=params(CACHE_MIB),
        cost_estimate=cost(10_000_000_000, slots * rows * size * 2),
        name="cache_attention",
    )(
        in_hbm(positions),
        in_hbm(queries),
        in_hbm(new_kv.reshape(slots, kv * 2, size)),
        in_hbm(response_cache.reshape(slots, rows, size)),
        in_hbm(prompt_hidden),
    )


def project_kernel(
    chunks, excess, hid, gain_ref, freq_ref, w_hbm, k_ref, v_ref, w, wide, acc, turn, wsem
):
    rows, width = hid.shape
    size = w.shape[1]
    ways = w.shape[0] // width
    depth = width // chunks
    loads = []
    for c in range(chunks):
        part = pl.ds(c * depth * ways, depth * ways)
        loads.append(pltpu.make_async_copy(w_hbm.at[part, :], w.at[part, :], wsem.at[c]))
        loads[-1].start()
    token = lax.axis_index("dev") * rows + lax.broadcasted_iota(jnp.int32, (rows, size), 0)
    offset, start = token, jnp.int32(0)
    for p in range(excess.shape[0]):
        offset = jnp.where(token >= start, token - start, offset)
        start = start + PROMPT_MIN + excess[p]
    lane = lax.broadcasted_iota(jnp.int32, (rows, size), 1)
    angle = offset.astype(jnp.float32) * freq_ref[...]
    turn[...] = jnp.cos(jnp.where(lane < size // 2, angle, angle - np.float32(np.pi / 2)))
    total = jnp.zeros((rows, 1), jnp.float32)
    for c in range(chunks):
        x = hid[:, c * depth : (c + 1) * depth].astype(jnp.float32)
        total = total + jnp.sum(x * x, axis=1, keepdims=True)
    inverse = lax.rsqrt(total / width + EPS)
    for c in range(chunks):
        at = slice(c * depth, (c + 1) * depth)
        x = hid[:, at].astype(jnp.float32) * inverse * gain_ref[:, at]
        x = x.astype(jnp.bfloat16)
        loads[c].wait()
        buffer = wide.at[c % 2]
        buffer[...] = w[c * depth * ways : (c + 1) * depth * ways, :].astype(jnp.float32)
        parts = [
            buffer[pl.ds(j, depth, stride=ways), :].astype(jnp.bfloat16) for j in range(ways)
        ]
        term = dot(x, jnp.concatenate(parts, axis=1), NN)
        if c == 0:
            acc[...] = term
        else:
            acc[...] += term
    first = lane < size // 2
    both = turn[...]
    swapped = pltpu.roll(both, size // 2, axis=1)
    cosine = jnp.where(first, both, swapped)
    sine = jnp.where(first, -swapped, both)
    for n in range(ways // 2):
        key = acc[:, 2 * n * size : (2 * n + 1) * size]
        turned = key * cosine + pltpu.roll(key, size // 2, axis=1) * sine
        k_ref[n] = turned.astype(k_ref.dtype)
        v_ref[n] = acc[:, (2 * n + 1) * size : (2 * n + 2) * size].astype(v_ref.dtype)


def project(prompt_hidden, norm_gain, kv_weight, prompt_excess):
    rows, width = prompt_hidden.shape
    kv, size = kv_weight.shape[1], kv_weight.shape[3]
    ways = kv * 2
    chunks = 8
    depth = width // chunks
    half = np.arange(size // 2, dtype=np.float64)
    freq = ROPE_BASE ** (-2.0 * half / size)
    freq = jnp.asarray(np.concatenate([freq, freq])[None, :], jnp.float32)
    f32, bf16 = jnp.float32, jnp.bfloat16
    return pl.pallas_call(
        functools.partial(project_kernel, chunks),
        in_specs=[SMEM, VMEM, VMEM, VMEM, HBM],
        out_specs=[VMEM, VMEM],
        out_shape=[jax.ShapeDtypeStruct((kv, rows, size), bf16)] * 2,
        scratch_shapes=[
            pltpu.VMEM((width * ways, size), bf16),
            pltpu.VMEM((2, depth * ways, size), f32),
            pltpu.VMEM((rows, ways * size), f32),
            pltpu.VMEM((rows, size), f32),
            pltpu.SemaphoreType.DMA((chunks,)),
        ],
        compiler_params=params(),
        cost_estimate=cost(10_000_000_000, width * (rows + ways * size) * 2),
        name="project",
    )(
        prompt_excess,
        prompt_hidden,
        norm_gain[None, :],
        freq,
        in_hbm(kv_weight.reshape(width * ways, size)),
    )


def pick_tile(refs, owner, phase, index):
    own = digit(lax.axis_index("dev"), phase)
    tile = refs[0][index]
    for k in range(1, len(refs)):
        tile = jnp.where(digit(owner, phase) == jnp.bitwise_xor(own, k), refs[k][index], tile)
    return tile


def slot_of(owner, counts, p, r, slots):
    return jnp.minimum(first_slot(owner, counts, p) + r, slots - 1)


def table_kernel(phase, raw, carried, owner, counts, *refs):
    radix = phase[1]
    sources, out = refs[:radix], refs[-1]
    entries = owner.shape[0] * RESP
    slots = sources[0].shape[0]
    for p in range(owner.shape[0]):
        for r in range(RESP):
            index = slot_of(owner, counts, p, r, slots) if raw else p * RESP + r
            out[p * RESP + r] = pick_tile(sources, owner[p], phase, index)
    at = entries
    if raw:
        local = refs[radix]
        out[at : at + local.shape[0]] = local[...]
    else:
        for source in sources:
            out[at : at + carried] = source[entries : entries + carried]
            at += carried


def make_table(phase, raw, carried, owner, counts, sources, local):
    heads, size = sources[0].shape[1:]
    entries = owner.shape[0] * RESP
    extra = local.shape[0] if raw else carried * len(sources)
    args = list(sources) + ([local] if raw else [])
    return pl.pallas_call(
        functools.partial(table_kernel, phase, raw, carried),
        in_specs=[SMEM, SMEM] + [VMEM] * len(args),
        out_specs=VMEM,
        out_shape=jax.ShapeDtypeStruct((entries + extra, heads, size), sources[0].dtype),
        compiler_params=params(),
        cost_estimate=cost(100_000_000, 200_000),
        name="make_table",
    )(owner, counts, *args)


def stat_rows(rows):
    return 16 * pl.cdiv(3 * pl.cdiv(rows, LANES), 16)


def put_state(out, mixed, lse, rows):
    out[:rows, :] = mixed.astype(out.dtype)
    count = pl.cdiv(rows, LANES)
    line = lax.broadcasted_iota(jnp.int32, (LANES, LANES), 0)
    lane = lax.broadcasted_iota(jnp.int32, (LANES, LANES), 1)
    place = lax.broadcasted_iota(jnp.int32, (stat_rows(rows), LANES), 0)
    stats = jnp.zeros((stat_rows(rows), LANES), jnp.float32)
    for b in range(count):
        size = min(LANES, rows - b * LANES)
        eye = line[:size] == lane[:size]
        rest = jnp.sum(
            jnp.where(eye, lse[b * LANES : b * LANES + size, :], 0.0), axis=0, keepdims=True
        )
        for k in range(3):
            term = rest.astype(jnp.bfloat16).astype(jnp.float32)
            stats = jnp.where(place == 3 * b + k, term, stats)
            rest = rest - term
    out[rows : rows + stat_rows(rows), :] = stats.astype(out.dtype)


def get_lse(message, rows):
    stats = message[rows : rows + stat_rows(rows), :].astype(jnp.float32)
    line = lax.broadcasted_iota(jnp.int32, (LANES, LANES), 0)
    lane = lax.broadcasted_iota(jnp.int32, (LANES, LANES), 1)
    blocks = []
    for b in range(pl.cdiv(rows, LANES)):
        size = min(LANES, rows - b * LANES)
        row = (stats[3 * b : 3 * b + 1] + stats[3 * b + 1 : 3 * b + 2]) + stats[3 * b + 2 : 3 * b + 3]
        eye = line[:size] == lane[:size]
        blocks.append(jnp.sum(jnp.where(eye, row, 0.0), axis=1, keepdims=True))
    return jnp.concatenate(blocks, axis=0) if len(blocks) > 1 else blocks[0]


def merge(messages, rows):
    lses = [get_lse(m, rows) for m in messages]
    peak = functools.reduce(jnp.maximum, lses)
    total = jnp.zeros_like(peak)
    mixed = None
    for m, lse in zip(messages, lses):
        weight = jnp.exp(lse - peak)
        total = total + weight
        term = m[:rows, :].astype(jnp.float32) * weight
        mixed = term if mixed is None else mixed + term
    return mixed / total, peak + jnp.log(total)


def prompt_kernel(
    phase, carried, excess, owner, counts, k_ref, v_ref, o_ref, lse_ref, *refs
):
    radix = phase[1]
    sources, out, pay, table, mine_o, mine_lse = refs[:radix], *refs[radix:]
    kv, tokens, size = k_ref.shape
    slots, heads, _ = o_ref.shape
    group = heads // kv
    prompts = owner.shape[0]
    rows = prompts * RESP * heads
    me = lax.axis_index("dev")
    for p in range(prompts):
        here = owner[p] == me
        for r in range(RESP):
            t = p * RESP + r
            slot = slot_of(owner, counts, p, r, slots)
            tile = pick_tile(sources, owner[p], phase, t)
            table[t * heads : (t + 1) * heads, :] = tile.astype(jnp.float32)
            mine_o[t * heads : (t + 1) * heads, :] = o_ref[slot]
            mine_lse[t * heads : (t + 1) * heads, :] = jnp.where(here, lse_ref[slot], LOW)
    queries = table[...].astype(jnp.bfloat16)
    head = (lax.broadcasted_iota(jnp.int32, (rows, 1), 0) % heads) // group
    scores = dot(queries, k_ref[0], NT)
    for n in range(1, kv):
        scores = jnp.where(head == n, dot(queries, k_ref[n], NT), scores)
    token = me * tokens + lax.broadcasted_iota(jnp.int32, (1, tokens), 1)
    start = jnp.int32(0)
    valid = []
    for p in range(prompts):
        end = start + PROMPT_MIN + excess[p]
        inside = ((token >= start) & (token < end)).astype(jnp.float32)
        valid.append(jnp.broadcast_to(inside, (RESP * heads, tokens)))
        start = end
    valid = jnp.concatenate(valid, axis=0) > 0.5
    scores = jnp.where(valid, scores * size ** (-0.5), LOW)
    peak = jnp.max(scores, axis=1, keepdims=True)
    weights = jnp.where(valid, jnp.exp(scores - peak), 0.0)
    total = jnp.sum(weights, axis=1, keepdims=True)
    weights = weights.astype(jnp.bfloat16)
    mixed = dot(weights, v_ref[0], NN)
    for n in range(1, kv):
        mixed = jnp.where(head == n, dot(weights, v_ref[n], NN), mixed)
    other = mine_lse[...]
    top = jnp.maximum(other, peak)
    left = jnp.exp(peak - top)
    right = jnp.exp(other - top)
    total = total * left + right
    mixed = (mixed * left + mine_o[...] * right) / total
    put_state(out, mixed, top + jnp.log(total), rows)
    entries = prompts * RESP
    for i, source in enumerate(sources):
        pay[i * carried : (i + 1) * carried] = source[entries : entries + carried]


def prompt_attention(phase, carried, excess, owner, counts, keys, values, o, lse, sources):
    heads, size = o.shape[1:]
    rows = owner.shape[0] * RESP * heads
    f32 = jnp.float32
    return pl.pallas_call(
        functools.partial(prompt_kernel, phase, carried),
        in_specs=[SMEM] * 3 + [VMEM] * (4 + len(sources)),
        out_specs=[VMEM, VMEM],
        out_shape=[
            jax.ShapeDtypeStruct((rows + stat_rows(rows), size), jnp.bfloat16),
            jax.ShapeDtypeStruct((carried * len(sources), heads, size), jnp.bfloat16),
        ],
        scratch_shapes=[pltpu.VMEM((rows, size), f32)] * 3,
        compiler_params=params(),
        cost_estimate=cost(2_000_000_000, 500_000),
        name="prompt_attention",
    )(excess, owner, counts, keys, values, o, lse, *sources)


def merge_kernel(rows, *refs):
    mixed, lse = merge(refs[:-1], rows)
    put_state(refs[-1], mixed, jnp.broadcast_to(lse, mixed.shape), rows)


def merge_states(rows, messages):
    size = messages[0].shape[1]
    return pl.pallas_call(
        functools.partial(merge_kernel, rows),
        in_specs=[VMEM] * len(messages),
        out_specs=VMEM,
        out_shape=jax.ShapeDtypeStruct((rows + stat_rows(rows), size), jnp.bfloat16),
        compiler_params=params(),
        cost_estimate=cost(1_000_000_000, 500_000),
        name="merge_states",
    )(*messages)


def base_kernel(offsets, slots, owner, counts, w_ref, *refs):
    sources, keep, give, pick, lhs = refs[:-4], *refs[-4:]
    heads, size, _ = w_ref.shape
    me = lax.axis_index("dev")
    block = slots * heads
    per = len(offsets) // len(sources)
    for i, offset in enumerate(offsets):
        at = pl.multiple_of(jnp.bitwise_xor(me, offset) * slots, slots)
        begin = (i % per) * block
        for h in range(heads):
            lhs[pl.ds(at, slots), h * size : (h + 1) * size] = sources[i // per][
                begin + h * slots : begin + (h + 1) * slots, :
            ]
    half = keep.shape[0]
    role = lax.axis_index("role")
    weight = w_ref[...].reshape(heads * size, w_ref.shape[2])
    keep[...] = dot(lhs[pl.ds(pl.multiple_of(role * half, half), half), :], weight, NN)
    give[...] = dot(lhs[pl.ds(pl.multiple_of((1 - role) * half, half), half), :], weight, NN)
    entry = lax.broadcasted_iota(jnp.int32, (1, pick.shape[1]), 1)
    row = jnp.full((1, pick.shape[1]), -1, jnp.int32)
    for p in range(owner.shape[0]):
        start = owner[p] * slots + first_slot(owner, counts, p) - role * half
        rank = entry - p * RESP
        live = (rank >= 0) & (rank < RESP) & (rank < counts[p])
        row = jnp.where(live, start + rank, row)
    line = lax.broadcasted_iota(jnp.int32, pick.shape, 0)
    pick[...] = jnp.where(line == row, 1.0, 0.0)


def base_product(offsets, slots, entries, owner, counts, weight, sources):
    heads, size, columns = weight.shape
    total = len(offsets) * slots
    half = jax.ShapeDtypeStruct((total // 2, columns), jnp.float32)
    return pl.pallas_call(
        functools.partial(base_kernel, offsets, slots),
        in_specs=[SMEM, SMEM] + [VMEM] * (1 + len(sources)),
        out_specs=[VMEM] * 3,
        out_shape=[half, half, jax.ShapeDtypeStruct((total // 2, entries), jnp.float32)],
        scratch_shapes=[pltpu.VMEM((total, heads * size), jnp.bfloat16)],
        compiler_params=params(),
        cost_estimate=cost(2_000_000_000, 1_000_000),
        name="base_product",
    )(owner, counts, weight, *sources)


def answer_kernel(rows, w_ref, *refs):
    messages, answers, part, joined = refs[:-3], *refs[-3:]
    heads = w_ref.shape[0]
    mixed, _ = merge(messages, rows)
    joined[...] = mixed
    answers[...] = mixed.astype(answers.dtype)
    total = None
    for h in range(heads):
        lhs = joined[pl.ds(h, rows // heads, stride=heads), :].astype(jnp.bfloat16)
        term = dot(lhs, w_ref[h], NN)
        total = term if total is None else total + term
    part[: rows // heads, :] = total
    rest = part.shape[0] - rows // heads
    if rest:
        part[rows // heads :, :] = jnp.zeros((rest, part.shape[1]), part.dtype)


def answer_product(rows, entries, weight, messages):
    heads, size, columns = weight.shape
    return pl.pallas_call(
        functools.partial(answer_kernel, rows),
        in_specs=[VMEM] * (1 + len(messages)),
        out_specs=[VMEM, VMEM],
        out_shape=[
            jax.ShapeDtypeStruct((rows, size), jnp.bfloat16),
            jax.ShapeDtypeStruct((entries, columns), jnp.float32),
        ],
        scratch_shapes=[pltpu.VMEM((rows, size), jnp.float32)],
        compiler_params=params(),
        cost_estimate=cost(1_000_000_000, 1_000_000),
        name="answer_product",
    )(weight, *messages)


def attended_kernel(owner, counts, o_ref, answers, out):
    slots = o_ref.shape[0]
    out[...] = o_ref[...].astype(out.dtype)
    me = lax.axis_index("dev")
    for p in range(owner.shape[0]):
        for r in range(RESP):

            @pl.when((owner[p] == me) & (r < counts[p]))
            def _():
                out[slot_of(owner, counts, p, r, slots)] = answers[p * RESP + r]


def attended_rows(owner, counts, o, answers):
    return pl.pallas_call(
        attended_kernel,
        in_specs=[SMEM, SMEM, VMEM, VMEM],
        out_specs=VMEM,
        out_shape=jax.ShapeDtypeStruct(o.shape, jnp.bfloat16),
        compiler_params=params(),
        cost_estimate=cost(500_000_000, 1_000_000),
        name="attended_rows",
    )(owner, counts, o, answers)


def finish_kernel(keep, taken, part, part_taken, pick, out):
    chosen = pick[...]
    fixed = part[...] + part_taken[...]
    patch = lax.dot_general(
        chosen, fixed, NN, precision=lax.Precision.HIGHEST, preferred_element_type=jnp.float32
    )
    answered = jnp.max(chosen, axis=1, keepdims=True) > 0.5
    out[...] = jnp.where(answered, patch, keep[...] + taken[...]).astype(out.dtype)


def finish(keep, taken, part, part_taken, pick):
    return pl.pallas_call(
        finish_kernel,
        in_specs=[VMEM] * 5,
        out_specs=VMEM,
        out_shape=jax.ShapeDtypeStruct(keep.shape, jnp.bfloat16),
        compiler_params=params(),
        name="finish",
    )(keep, taken, part, part_taken, pick)


def swap_role(x):
    return lax.ppermute(x, "role", [(0, 1), (1, 0)])


def on_device(
    prompt_hidden,
    norm_gain,
    kv_weight,
    excess,
    owner,
    counts,
    queries,
    new_kv,
    response_cache,
    positions,
    out_weight,
):
    slots, heads, size = queries.shape
    steps = phases(lax.axis_size("dev"))
    rows = owner.shape[0] * RESP * heads
    received = [queries] + exchange(queries, steps[0])
    local, o, lse, hidden = cache_attention(
        positions, queries, new_kv, response_cache, prompt_hidden
    )
    local = local.reshape(slots, heads, size)
    offsets = [0]
    carried = slots
    raw = True
    for before, phase in zip(steps[:-1], steps[1:]):
        message = make_table(before, raw, carried, owner, counts, received, local)
        received = [message] + exchange(message, phase)
        carried = carried if raw else carried * before[1]
        offsets = [k * phase[0] ^ a for k in range(phase[1]) for a in offsets]
        raw = False
    keys, values = project(hidden, norm_gain, kv_weight, excess)
    message, payload = prompt_attention(
        steps[-1], carried, excess, owner, counts, keys, values, o, lse, received
    )
    payload = payload.reshape(-1, size)
    received = [message] + exchange(message, steps[0])
    blocks = [payload] + exchange(payload, steps[0])
    offsets = [k * steps[0][0] ^ a for k in range(steps[0][1]) for a in offsets]
    for phase in steps[1:]:
        message = merge_states(rows, received)
        received = [message] + exchange(message, phase)
    entries = 8 * pl.cdiv(rows // heads, 8)
    keep, give, pick = base_product(offsets, slots, entries, owner, counts, out_weight, blocks)
    taken = swap_role(give)
    answers, part = answer_product(rows, entries, out_weight, received)
    part_taken = swap_role(part)
    attended = attended_rows(owner, counts, o, answers.reshape(-1, heads, size))
    block_out = finish(keep, taken, part, part_taken, pick)
    return (attended, block_out)


def solution(mesh):
    return jax.shard_map(
        on_device,
        mesh=mesh,
        in_specs=(
            P(("groups", "dev"), None),
            P(),
            P(None, "role", None, None),
            P("groups"),
            P("groups"),
            P("groups"),
            P(("groups", "dev"), "role", None),
            P(("groups", "dev"), "role", None, None),
            P(("groups", "dev"), None, "role", None, None),
            P(("groups", "dev")),
            P("role", None, "dev"),
        ),
        out_specs=(P(("groups", "dev"), "role", None), P(("groups", "role"), "dev")),
        check_vma=False,
    )
```
